128 devices in a mesh: tm: 128 (over z, y, x, core).
Axes of the slice: x: 4, y: 4, z: 4, core: 2. Of those that a mesh axis runs over, the one named last changes fastest.
Arguments:
- krylov_basis: float32 [8, 512, 32, 512], P(None, 'tm'), may hold values from -6 to 6, as said below
- vector: float32 [512, 32, 512], P('tm'), may hold values from -60 to 60
- conductance: float32 [32, 512], replicated, may hold values from 1e-05 to 0.3
Outputs:
- preconditioned: float32 [512, 32, 512], P('tm')
- next_vector: float32 [512, 32, 512], P('tm')
- coefficients: float32 [9], replicated
The draws below stay inside these ranges and needn't reach their ends.
Inputs may be any that keep to these rules, and one draw needn't show every extreme that they name: `krylov_basis`: the 8 fields are orthonormal, up to float32 rounding, under the mean over all cells of their product.
All inputs are finite; a program needn't handle non-finite values.
Results may differ from the reference program's by a relative error of at most 0.0003.
Values sent between devices are 32-bit elements.
No kernel may reach another device: no remote copies, remote signals or barrier semaphores. Data moves between devices by JAX's collectives and lax.ppermute only.
A program may use at most 64 MiB of HBM per device.

```python
import jax
import jax.numpy as jnp
from jax import lax

SX = 32
SY = 512
LEVELS = 3
KPRIOR = 8
NT = 512


def orthonormal_fields(key):
    cell_count = NT * SX * SY
    raw_fields = jnp.clip(jax.random.normal(jax.random.fold_in(key, 11), (KPRIOR, NT, SX, SY), jnp.float32), -4.5, 4.5)
    members = []
    for position in range(KPRIOR):
        current = raw_fields[position]
        for sweep_at in range(2):
            for earlier in members:
                current = current - jnp.sum(current * earlier) / cell_count * earlier
        current = current / jnp.sqrt(jnp.sum(current * current) / cell_count)
        members.append(current)
    return jnp.stack(members)


def draw_krylov_basis(key, part):
    return orthonormal_fields(key)


def draw_vector(key, part):
    members = orthonormal_fields(key)
    magnitude = jax.random.uniform(jax.random.fold_in(key, 23), (KPRIOR,), jnp.float32, 0.5, 1.5)
    flips = jnp.where(jax.random.bernoulli(jax.random.fold_in(key, 29), 0.5, (KPRIOR,)), 1.0, -1.0)
    remainder = 0.6 * jnp.clip(jax.random.normal(jax.random.fold_in(key, 31), (NT, SX, SY), jnp.float32), -4.0, 4.0)
    mixed = jnp.einsum('k,kabc->abc', magnitude * flips, members, precision=lax.Precision.HIGHEST)
    return mixed + remainder


def draw_conductance(key, part):
    low_log = jnp.log(jnp.float32(1e-05))
    high_log = jnp.log(jnp.float32(0.3))
    return jnp.exp(jax.random.uniform(jax.random.fold_in(key, 43), (SX, SY), jnp.float32, low_log, high_log))


def setup_inputs(seed: int = 0) -> dict:
    seeds = jax.random.split(jax.random.key(seed), 4)
    return {
        "krylov_basis": draw_krylov_basis(jax.random.fold_in(seeds[3], 71), 0),
        "vector": draw_vector(jax.random.fold_in(seeds[3], 71), 0),
        "conductance": draw_conductance(jax.random.fold_in(seeds[3], 71), 0),
    }


OMEGA = 0.7
FLOOR = 0.25

def beside(volume):
    padded = jnp.pad(volume, ((0, 0), (1, 1), (1, 1)))
    return padded[:, 2:, 1:-1] + padded[:, :-2, 1:-1] + padded[:, 1:-1, 2:] + padded[:, 1:-1, :-2]

def spatial(volume, conduct):
    return volume + conduct * (4.0 * volume - beside(volume))

def time_operator(volume, conduct):
    earlier = jnp.concatenate([jnp.zeros_like(volume[:1]), volume[:-1]], axis=0)
    return spatial(volume, conduct) - earlier

def block_inverse(source, conduct):
    diagonal = 1.0 + 4.0 * conduct
    sweep_one = source / diagonal
    return (source + conduct * beside(sweep_one)) / diagonal

def coarse_march(source, conduct):
    diagonal = 1.0 + 4.0 * conduct

    def advance(carry_state, slab_in):
        carry_state = (slab_in + carry_state) / diagonal
        return (carry_state, carry_state)
    return lax.scan(advance, jnp.zeros_like(conduct), source)[1]

def vcycle(source, conduct, level_at):
    if level_at == LEVELS - 1:
        return coarse_march(source, conduct)
    smooth = OMEGA * block_inverse(source, conduct)
    remain = source - time_operator(smooth, conduct)
    coarse = remain[0::2] + remain[1::2]
    correction = vcycle(coarse, 2.0 * conduct, level_at + 1)
    smooth = smooth + jnp.repeat(correction, 2, axis=0)
    return smooth + OMEGA * block_inverse(source - time_operator(smooth, conduct), conduct)

def reference(krylov_basis, vector, conductance):
    cell_count = NT * SX * SY
    preconditioned = vcycle(vector, conductance, 0)
    applied = time_operator(preconditioned, conductance)
    weights = []
    for member in range(KPRIOR):
        weight = jnp.sum(applied * krylov_basis[member]) / cell_count
        applied = applied - weight * krylov_basis[member]
        weights.append(weight)
    length = jnp.sqrt(jnp.sum(applied * applied) / cell_count)
    next_vector = applied / jnp.maximum(length, FLOOR)
    coefficients = jnp.stack(weights + [length])
    return (preconditioned, next_vector, coefficients)
```

```python
import functools

import jax
import jax.numpy as jnp
from jax import lax
from jax.experimental import pallas as pl
from jax.experimental.pallas import tpu as pltpu
from jax.sharding import PartitionSpec as P

TM = "tm"
OMEGA = 0.7
FLOOR = 0.25
ROWS, LANES = 8, 128
VMEM = pltpu.VMEM


class Grid:
    def __init__(self, conduct):
        sx, sy = conduct.shape
        row = lax.broadcasted_iota(jnp.int32, (sx, sy), 0)
        col = lax.broadcasted_iota(jnp.int32, (sx, sy), 1)
        self.sx, self.sy = sx, sy
        self.first_row, self.last_row = row == 0, row == sx - 1
        self.first_col, self.last_col = col == 0, col == sy - 1
        self.conduct = conduct

    def beside(self, v):
        zero = jnp.zeros_like(v)
        above = jnp.where(self.first_row, zero, pltpu.roll(v, 1, 0))
        below = jnp.where(self.last_row, zero, pltpu.roll(v, self.sx - 1, 0))
        left = jnp.where(self.first_col, zero, pltpu.roll(v, 1, 1))
        right = jnp.where(self.last_col, zero, pltpu.roll(v, self.sy - 1, 1))
        return (above + below) + (left + right)

    def level(self, scale):
        return Level(self, scale)


class Level:
    def __init__(self, grid, scale):
        self.grid = grid
        self.c = scale * grid.conduct
        self.diag = 1.0 + 4.0 * self.c
        self.inv = 1.0 / self.diag
        self.winv = OMEGA * self.inv

    def K(self, v):
        return self.diag * v - self.c * self.grid.beside(v)

    def S(self, r):
        return (r + self.c * self.grid.beside(r * self.inv)) * self.winv

    def T(self, v):
        return v + self.S(v - self.K(v))


def tiles(sx, sy):
    for i in range(sx // ROWS):
        for l in range(sy // LANES):
            yield (i * (sy // LANES) + l), slice(ROWS * i, ROWS * (i + 1)), slice(LANES * l, LANES * (l + 1))


def down_kernel(r_ref, c_ref, f_ref, d_ref, halo_ref, x_ref, keep_ref, ct_ref):
    sx, sy = c_ref.shape
    grid = Grid(c_ref[...])
    fine, mid = grid.level(1.0), grid.level(2.0)
    diag2 = 1.0 + 16.0 * c_ref[...]
    r = [r_ref[t] for t in range(4)]
    u = [fine.S(r[t]) for t in range(4)]
    rho0 = r[0] + r[1] - fine.K(u[0] + u[1]) + u[0]
    rho1 = r[2] + r[3] - fine.K(u[2] + u[3]) + u[1] + u[2]
    x = u[3]
    v0 = mid.S(rho0)
    v1 = mid.S(rho1)
    vs = v0 + v1
    loc = rho0 + rho1 - mid.K(vs) + v0
    sx_ = mid.S(x)
    g = x + v1 + sx_ - mid.K(sx_)
    f = loc / diag2 + g
    for t, rows, cols in tiles(sx, sy):
        f_ref[t * ROWS : (t + 1) * ROWS, :] = f[rows, cols]
        ct_ref[t * ROWS : (t + 1) * ROWS, :] = c_ref[rows, cols]
    me = lax.axis_index(TM)
    d_ref[...] = 1.0 / (1.0 + 16.0 * ct_ref[pl.ds(me, 1), :])
    alpha = v1 + mid.S(rho1 - mid.K(v1) + v0) - mid.T(g)
    beta = x + fine.S(r[3] - fine.K(x) + u[2])
    halo_ref[0] = x
    halo_ref[1] = alpha
    halo_ref[2] = beta
    x_ref[...] = x
    for t in range(4):
        keep_ref[t] = u[t]
    keep_ref[4] = rho0
    keep_ref[5] = rho1
    keep_ref[6] = loc


def scan_kernel(f_ref, d_ref, e_ref):
    count = f_ref.shape[0]
    row = lax.broadcasted_iota(jnp.int32, (ROWS, LANES), 0)
    d1 = jnp.broadcast_to(d_ref[...], (ROWS, LANES))
    d2 = d1 * d1
    d4 = d2 * d2
    d8 = d4 * d4
    one = jnp.ones_like(d1)
    power = (
        jnp.where((row & 1) > 0, d1, one)
        * jnp.where((row & 2) > 0, d2, one)
        * jnp.where((row & 4) > 0, d4, one)
    )
    carry = jnp.zeros((ROWS, LANES), jnp.float32)

    def shifted(v, by):
        return jnp.where(row < by, 0.0, pltpu.roll(v, by, 0))

    blocks = []
    for b in range(count // ROWS):
        y = f_ref[b * ROWS : (b + 1) * ROWS, :]
        y = y + d1 * shifted(y, 1)
        y = y + d2 * shifted(y, 2)
        y = y + d4 * shifted(y, 4)
        blocks.append(y)
    for b, y in enumerate(blocks):
        e_ref[b * ROWS : (b + 1) * ROWS, :] = shifted(y, 1) + power * carry
        carry = jnp.broadcast_to(y[ROWS - 1 : ROWS, :], (ROWS, LANES)) + d8 * carry


def up_kernel(e_ref, r_ref, c_ref, halo_ref, far_ref, keep_ref, q_hbm, p_ref, w_ref, dots_ref, q_ref, ef_ref, sem):
    copy = pltpu.make_async_copy(q_hbm, q_ref, sem)
    copy.start()
    sx, sy = c_ref.shape
    for t, rows, cols in tiles(sx, sy):
        ef_ref[rows, cols] = e_ref[t * ROWS : (t + 1) * ROWS, :]
    grid = Grid(c_ref[...])
    fine, mid = grid.level(1.0), grid.level(2.0)
    diag2 = 1.0 + 16.0 * c_ref[...]
    entry = ef_ref[...]
    x = halo_ref[0]
    rho0 = keep_ref[4] + x
    rho1 = keep_ref[5]
    m = (keep_ref[6] + entry) / diag2
    v0 = mid.S(rho0) + m
    v1 = mid.S(rho1) + m
    xs = mid.S(x)
    before = entry - (x + xs - mid.K(xs))
    q0 = v0 + mid.S(rho0 - mid.K(v0) + before)
    q1 = v1 + mid.S(rho1 - mid.K(v1) + v0)
    qb = halo_ref[1] + mid.S(mid.S(far_ref[...])) + mid.T(entry)
    ub = x + qb
    pb = halo_ref[2] + fine.T(qb)
    nine = [jnp.zeros((ROWS, LANES), jnp.float32) for _ in range(9)]
    q = (q0, q0, q1, q1)
    for t in range(4):
        u = keep_ref[t] + q[t]
        p = u + fine.S(r_ref[t] - fine.K(u) + ub)
        p_ref[t] = p
        w_ref[t] = fine.K(p) - pb
        ub, pb = u, p
    copy.wait()
    for t in range(4):
        for _, rows, cols in tiles(sx, sy):
            w = w_ref[t, rows, cols]
            for k in range(8):
                nine[k] = nine[k] + w * q_ref[k, t, rows, cols]
            nine[8] = nine[8] + w * w
    lane = lax.broadcasted_iota(jnp.int32, (ROWS, LANES), 1)
    out = jnp.zeros((ROWS, LANES), jnp.float32)
    for k in range(9):
        out = jnp.where(lane == k, jnp.sum(nine[k], axis=(0, 1), keepdims=True), out)
    for b in range(dots_ref.shape[0] // ROWS):
        dots_ref[b * ROWS : (b + 1) * ROWS, :] = out


def two_sum(a, b):
    total = a + b
    part = total - a
    return total, (a - (total - part)) + (b - part)


def two_square(a):
    big = a * 4097.0
    high = big - (big - a)
    low = a - high
    square = a * a
    return square, ((high * high - square) + 2.0 * high * low) + low * low


def pair_add(a, b):
    high, low = two_sum(a[0], b[0])
    return high, low + (a[1] + b[1])


def finish_kernel(cells, dots_ref, w_ref, q_hbm, next_ref, coef_ref, q_ref, sem):
    copy = pltpu.make_async_copy(q_hbm, q_ref, sem)
    copy.start()
    parts = [(dots_ref[b * ROWS : (b + 1) * ROWS, :], jnp.zeros((ROWS, LANES), jnp.float32)) for b in range(dots_ref.shape[0] // ROWS)]
    while len(parts) > 1:
        parts = [pair_add(parts[2 * i], parts[2 * i + 1]) for i in range(len(parts) // 2)]
    pair = parts[0]
    for by in (4, 2, 1):
        pair = pair_add(pair, (pltpu.roll(pair[0], by, 0), pltpu.roll(pair[1], by, 0)))
    high, low = two_sum(pair[0] / cells, pair[1] / cells)
    lane = lax.broadcasted_iota(jnp.int32, (ROWS, LANES), 1)
    sq, sq_low = two_square(high)
    is_h = lane < 8
    is_s = lane == 8
    zero = jnp.zeros_like(high)
    rest = (
        jnp.where(is_h, -sq, jnp.where(is_s, high, zero)),
        jnp.where(is_h, -(sq_low + 2.0 * high * low), jnp.where(is_s, low, zero)),
    )
    for by in (8, 4, 2, 1):
        rest = pair_add(rest, (pltpu.roll(rest[0], LANES - by, 1), pltpu.roll(rest[1], LANES - by, 1)))
    square = jnp.broadcast_to((rest[0] + rest[1])[:, 0:1], (ROWS, LANES))
    length = jnp.sqrt(jnp.maximum(square, 0.0))
    scale = 1.0 / jnp.maximum(length, FLOOR)
    coef = jnp.where(is_s, length, high)
    coef_ref[...] = coef[0, :9]
    h = [jnp.broadcast_to(high[:, k : k + 1], (ROWS, LANES)) for k in range(8)]
    copy.wait()
    steps, sx, sy = w_ref.shape
    for t in range(steps):
        for _, rows, cols in tiles(sx, sy):
            w = w_ref[t, rows, cols]
            for k in range(8):
                w = w - h[k] * q_ref[k, t, rows, cols]
            next_ref[t, rows, cols] = w * scale


def whole(n):
    return [pl.BlockSpec(memory_space=VMEM)] * n


def f32(*shape):
    return jax.ShapeDtypeStruct(shape, jnp.float32)


def on_device(krylov_basis, vector, conductance):
    count = lax.axis_size(TM)
    steps, sx, sy = vector.shape
    cells = float(steps * count * sx * sy)
    rows = sx * sy // LANES
    limit = pltpu.CompilerParams(vmem_limit_bytes=24 * 2**20)

    f, d, halo, x, keep = pl.pallas_call(
        down_kernel,
        out_shape=(f32(rows, LANES), f32(1, LANES), f32(3, sx, sy), f32(sx, sy), f32(7, sx, sy)),
        in_specs=whole(2),
        out_specs=tuple(whole(5)),
        scratch_shapes=[VMEM((rows, LANES), jnp.float32)],
        compiler_params=limit,
        name="down",
    )(vector, conductance)
    halo = lax.ppermute(halo, TM, [(k, k + 1) for k in range(count - 1)])
    far = lax.ppermute(x, TM, [(k, k + 2) for k in range(count - 2)])
    f = lax.all_to_all(f, TM, 0, 0, tiled=True)
    e = pl.pallas_call(
        scan_kernel,
        out_shape=f32(rows, LANES),
        in_specs=whole(2),
        out_specs=whole(1)[0],
        compiler_params=limit,
        name="scan",
    )(f, d)
    e = lax.all_to_all(e, TM, 0, 0, tiled=True)
    p, w, dots = pl.pallas_call(
        up_kernel,
        out_shape=(f32(steps, sx, sy), f32(steps, sx, sy), f32(count, LANES)),
        in_specs=whole(6) + [pl.BlockSpec(memory_space=pl.ANY)],
        out_specs=tuple(whole(3)),
        scratch_shapes=[
            VMEM(krylov_basis.shape, jnp.float32),
            VMEM((sx, sy), jnp.float32),
            pltpu.SemaphoreType.DMA,
        ],
        compiler_params=limit,
        name="up",
    )(e, vector, conductance, halo, far, keep, krylov_basis)
    dots = lax.all_to_all(dots, TM, 0, 0, tiled=True)
    following, coefficients = pl.pallas_call(
        functools.partial(finish_kernel, cells),
        out_shape=(f32(steps, sx, sy), f32(9)),
        in_specs=whole(2) + [pl.BlockSpec(memory_space=pl.ANY)],
        out_specs=tuple(whole(2)),
        scratch_shapes=[VMEM(krylov_basis.shape, jnp.float32), pltpu.SemaphoreType.DMA],
        compiler_params=limit,
        name="finish",
    )(dots, w, krylov_basis)
    return (p, following, coefficients)


def solution(mesh):
    return jax.shard_map(
        on_device,
        mesh=mesh,
        in_specs=(P(None, TM, None, None), P(TM, None, None), P()),
        out_specs=(P(TM, None, None), P(TM, None, None), P()),
        check_vma=False,
    )
```

```python
import functools

import jax
import jax.numpy as jnp
from jax import lax
from jax.experimental import pallas as pl
from jax.experimental.pallas import tpu as pltpu
from jax.sharding import PartitionSpec as P


TM = "tm"
OMEGA = 0.7
FLOOR = 0.25
ROWS, LANES = 8, 128
VMEM = pltpu.VMEM


class Grid:
    def __init__(self, conduct):
        sx, sy = conduct.shape
        row = lax.broadcasted_iota(jnp.int32, (sx, sy), 0)
        col = lax.broadcasted_iota(jnp.int32, (sx, sy), 1)
        self.sx, self.sy = sx, sy
        self.first_row, self.last_row = row == 0, row == sx - 1
        self.first_col, self.last_col = col == 0, col == sy - 1
        self.conduct = conduct

    def beside(self, v):
        zero = jnp.zeros_like(v)
        above = jnp.where(self.first_row, zero, pltpu.roll(v, 1, 0))
        below = jnp.where(self.last_row, zero, pltpu.roll(v, self.sx - 1, 0))
        left = jnp.where(self.first_col, zero, pltpu.roll(v, 1, 1))
        right = jnp.where(self.last_col, zero, pltpu.roll(v, self.sy - 1, 1))
        return (above + below) + (left + right)

    def level(self, scale):
        return Level(self, scale)


class Level:
    def __init__(self, grid, scale):
        self.grid = grid
        self.c = scale * grid.conduct
        self.diag = 1.0 + 4.0 * self.c
        self.inv = 1.0 / self.diag
        self.winv = OMEGA * self.inv

    def K(self, v):
        return self.diag * v - self.c * self.grid.beside(v)

    def S(self, r):
        return (r + self.c * self.grid.beside(r * self.inv)) * self.winv

    def T(self, v):
        return v + self.S(v - self.K(v))


def tiles(sx, sy):
    for i in range(sx // ROWS):
        for l in range(sy // LANES):
            yield (i * (sy // LANES) + l), slice(ROWS * i, ROWS * (i + 1)), slice(LANES * l, LANES * (l + 1))


def every_other(tile, which):
    return pl.ds(2 * ROWS * tile + which, ROWS, stride=2)


def down_kernel(r_hbm, c_hbm, f_ref, d_ref, r_ref, c_ref, u_ref, keep_ref, mid_ref, ct_ref, sems):
    copies = [pltpu.make_async_copy(r_hbm, r_ref, sems.at[0]), pltpu.make_async_copy(c_hbm, c_ref, sems.at[1])]
    for copy in copies:
        copy.start()
    for copy in copies:
        copy.wait()
    sx, sy = c_ref.shape
    grid = Grid(c_ref[...])
    fine, mid = grid.level(1.0), grid.level(2.0)
    r = [r_ref[t] for t in range(4)]
    u = [fine.S(r[t]) for t in range(4)]
    for t in range(4):
        u_ref[t] = u[t]
    rho0 = r[0] + r[1] - fine.K(u[0] + u[1]) + u[0]
    rho1 = r[2] + r[3] - fine.K(u[2] + u[3]) + u[1] + u[2]
    v0 = mid.S(rho0)
    v1 = mid.S(rho1)
    xs = mid.S(u[3])
    g = u[3] + v1 + xs - mid.K(xs)
    part = (rho0 + rho1 - mid.K(v0 + v1) + v0) / (1.0 + 16.0 * grid.conduct)
    f = part + g
    xss = mid.S(xs)
    for t, rows, cols in tiles(sx, sy):
        f_ref[every_other(t, 0), :] = f[rows, cols]
        f_ref[every_other(t, 1), :] = xss[rows, cols]
        ct_ref[t * ROWS : (t + 1) * ROWS, :] = c_ref[rows, cols]
    me = lax.axis_index(TM)
    d_ref[...] = 1.0 / (1.0 + 16.0 * ct_ref[pl.ds(me, 1), :])
    for k, field in enumerate((rho0, rho1, part)):
        keep_ref[k] = field
    for k, field in enumerate((v0, v1, g)):
        mid_ref[k] = field


def halo_kernel(r_ref, c_ref, u_ref, keep_ref, mid_ref, halo_ref):
    grid = Grid(c_ref[...])
    fine, mid = grid.level(1.0), grid.level(2.0)
    x = u_ref[3]
    rho1, v0, v1 = keep_ref[1], mid_ref[0], mid_ref[1]
    halo_ref[0] = x
    halo_ref[1] = v1 + mid.S(rho1 - mid.K(v1) + v0) - mid.T(mid_ref[2])
    halo_ref[2] = x + fine.S(r_ref[3] - fine.K(x) + u_ref[2])


def early_kernel(r_hbm, c_ref, u_ref, keep_ref, halo_ref, q_hbm, p_ref, w_ref, q_ref, r_ref, sems):
    fetch = pltpu.make_async_copy(r_hbm, r_ref, sems.at[1])
    fetch.start()
    copy = pltpu.make_async_copy(q_hbm, q_ref, sems.at[0])
    copy.start()
    grid = Grid(c_ref[...])
    fine, mid = grid.level(1.0), grid.level(2.0)
    x = halo_ref[0]
    part = keep_ref[2]
    xs = mid.S(x)
    rho0, rho1 = keep_ref[0] + x, keep_ref[1]
    v0 = mid.S(rho0) + part
    v1 = mid.S(rho1) + part
    q0 = v0 + mid.S(rho0 - mid.K(v0) - (x + xs - mid.K(xs)))
    q1 = v1 + mid.S(rho1 - mid.K(v1) + v0)
    qb = halo_ref[1]
    ub = x + qb
    pb = halo_ref[2] + fine.T(qb)
    q = (q0, q0, q1, q1)
    fetch.wait()
    for t in range(4):
        u = u_ref[t] + q[t]
        p = u + fine.S(r_ref[t] - fine.K(u) + ub)
        p_ref[t] = p
        w_ref[t] = fine.K(p) - pb
        ub, pb = u, p
    copy.wait()


def scan_kernel(f_ref, d_ref, e_ref):
    count = f_ref.shape[0] // 2
    row = lax.broadcasted_iota(jnp.int32, (ROWS, LANES), 0)
    d1 = jnp.broadcast_to(d_ref[...], (ROWS, LANES))
    d2 = d1 * d1
    d4 = d2 * d2
    d8 = d4 * d4
    one = jnp.ones_like(d1)
    power = (
        jnp.where((row & 1) > 0, d1, one)
        * jnp.where((row & 2) > 0, d2, one)
        * jnp.where((row & 4) > 0, d4, one)
    )
    carry = jnp.zeros((ROWS, LANES), jnp.float32)

    def shifted(v, by):
        return jnp.where(row < by, 0.0, pltpu.roll(v, by, 0))

    blocks = []
    for b in range(count // ROWS):
        y = f_ref[every_other(b, 0), :]
        y = y + d1 * shifted(y, 1)
        y = y + d2 * shifted(y, 2)
        y = y + d4 * shifted(y, 4)
        blocks.append(y)
    for b, y in enumerate(blocks):
        e_ref[every_other(b, 0), :] = shifted(y, 1) + power * carry
        carry = jnp.broadcast_to(y[ROWS - 1 : ROWS, :], (ROWS, LANES)) + d8 * carry
    last = jnp.zeros((ROWS, LANES), jnp.float32)
    for b in range(count // ROWS):
        far = pltpu.roll(f_ref[every_other(b, 1), :], 2, 0)
        e_ref[every_other(b, 1), :] = jnp.where(row < 2, last, far)
        last = far


def up_kernel(e_ref, c_ref, pe_ref, we_ref, q_ref, p_ref, w_ref, dots_ref, ef_ref, far_ref):
    sx, sy = c_ref.shape
    for t, rows, cols in tiles(sx, sy):
        ef_ref[rows, cols] = e_ref[every_other(t, 0), :]
        far_ref[rows, cols] = e_ref[every_other(t, 1), :]
    grid = Grid(c_ref[...])
    fine, mid = grid.level(1.0), grid.level(2.0)
    entry = ef_ref[...]
    m = entry / (1.0 + 16.0 * grid.conduct)
    mk = mid.K(m)
    q0 = m + mid.S(entry - mk)
    q1 = m + mid.S(m - mk)
    qb = mid.T(entry) + far_ref[...]
    k0, k1 = fine.K(q0), fine.K(q1)
    before = qb + fine.S(qb - fine.K(qb))
    for t, base, source in ((0, q0, qb - k0), (1, q0, q0 - k0), (2, q1, q0 - k1), (3, q1, q1 - k1)):
        p = base + fine.S(source)
        p_ref[t] = pe_ref[t] + p
        w_ref[t] = we_ref[t] + (fine.K(p) - before)
        before = p
    nine = [jnp.zeros((ROWS, LANES), jnp.float32) for _ in range(9)]
    for t in range(4):
        for _, rows, cols in tiles(sx, sy):
            w = w_ref[t, rows, cols]
            for k in range(8):
                nine[k] = nine[k] + w * q_ref[k, t, rows, cols]
            nine[8] = nine[8] + w * w
    lane = lax.broadcasted_iota(jnp.int32, (ROWS, LANES), 1)
    out = jnp.zeros((ROWS, LANES), jnp.float32)
    for k in range(9):
        out = jnp.where(lane == k, jnp.sum(nine[k], axis=(0, 1), keepdims=True), out)
    for b in range(dots_ref.shape[0] // ROWS):
        dots_ref[b * ROWS : (b + 1) * ROWS, :] = out


def two_sum(a, b):
    total = a + b
    part = total - a
    return total, (a - (total - part)) + (b - part)


def two_square(a):
    big = a * 4097.0
    high = big - (big - a)
    low = a - high
    square = a * a
    return square, ((high * high - square) + 2.0 * high * low) + low * low


def pair_add(a, b):
    high, low = two_sum(a[0], b[0])
    return high, low + (a[1] + b[1])


def finish_kernel(cells, dots_ref, w_ref, q_ref, p_ref, p_hbm, next_hbm, coef_hbm, next_ref, coef_ref, sems):
    copies = [pltpu.make_async_copy(p_ref, p_hbm, sems.at[0])]
    copies[0].start()
    parts = [(dots_ref[b * ROWS : (b + 1) * ROWS, :], jnp.zeros((ROWS, LANES), jnp.float32)) for b in range(dots_ref.shape[0] // ROWS)]
    while len(parts) > 1:
        parts = [pair_add(parts[2 * i], parts[2 * i + 1]) for i in range(len(parts) // 2)]
    pair = parts[0]
    for by in (4, 2, 1):
        pair = pair_add(pair, (pltpu.roll(pair[0], by, 0), pltpu.roll(pair[1], by, 0)))
    high, low = two_sum(pair[0] / cells, pair[1] / cells)
    lane = lax.broadcasted_iota(jnp.int32, (ROWS, LANES), 1)
    sq, sq_low = two_square(high)
    is_h = lane < 8
    is_s = lane == 8
    zero = jnp.zeros_like(high)
    rest = (
        jnp.where(is_h, -sq, jnp.where(is_s, high, zero)),
        jnp.where(is_h, -(sq_low + 2.0 * high * low), jnp.where(is_s, low, zero)),
    )
    for by in (8, 4, 2, 1):
        rest = pair_add(rest, (pltpu.roll(rest[0], LANES - by, 1), pltpu.roll(rest[1], LANES - by, 1)))
    square = jnp.broadcast_to((rest[0] + rest[1])[:, 0:1], (ROWS, LANES))
    length = jnp.sqrt(jnp.maximum(square, 0.0))
    scale = 1.0 / jnp.maximum(length, FLOOR)
    coef = jnp.where(is_s, length, high)
    coef_ref[...] = coef[0, :9]
    copies.append(pltpu.make_async_copy(coef_ref, coef_hbm, sems.at[1]))
    copies[1].start()
    h = [jnp.broadcast_to(high[:, k : k + 1], (ROWS, LANES)) for k in range(8)]
    steps, sx, sy = w_ref.shape
    for t in range(steps):
        for _, rows, cols in tiles(sx, sy):
            w = w_ref[t, rows, cols]
            for k in range(8):
                w = w - h[k] * q_ref[k, t, rows, cols]
            next_ref[t, rows, cols] = w * scale
        copies.append(pltpu.make_async_copy(next_ref.at[t], next_hbm.at[t], sems.at[2 + t]))
        copies[-1].start()
    for copy in copies:
        copy.wait()


def f32(*shape):
    return jax.ShapeDtypeStruct(shape, jnp.float32)


def held(*shape):
    return pltpu.VMEM(shape, jnp.float32)


IN_HBM = pl.BlockSpec(memory_space=pltpu.HBM)
IN_VMEM = pl.BlockSpec(memory_space=VMEM)


def call(kernel, ins, outs, scratch=(), cost=2**21):
    def run(*args):
        args = [pltpu.with_memory_space_constraint(a, pltpu.HBM) if s is IN_HBM else a for a, s in zip(args, ins)]
        return pl.pallas_call(
            kernel,
            out_shape=tuple(shape for shape, _ in outs),
            in_specs=list(ins),
            out_specs=tuple(spec for _, spec in outs),
            scratch_shapes=list(scratch),
            compiler_params=pltpu.CompilerParams(vmem_limit_bytes=16 * 2**20),
            cost_estimate=pl.CostEstimate(flops=cost, bytes_accessed=2**20, transcendentals=0),
        )(*args)

    return run


def exchanged(value):
    count = lax.axis_size(TM)
    pieces = value.reshape(count, value.shape[0] // count, LANES)
    return lax.all_to_all(pieces, TM, 0, 0, tiled=True).reshape(value.shape)


def passed(value, by, count):
    return lax.ppermute(value, TM, [(k, k + by) for k in range(count - by)])


def on_device(krylov_basis, vector, conductance):
    count = lax.axis_size(TM)
    steps, sx, sy = vector.shape
    cells = float(steps * count * sx * sy)
    rows = sx * sy // LANES
    slab = held(steps, sx, sy)
    out = pltpu.HBM((steps, sx, sy), jnp.float32)
    dma = pltpu.SemaphoreType.DMA

    f, d, r, c, u, keep, mid = call(
        down_kernel,
        [IN_HBM] * 2,
        [
            (s, IN_VMEM)
            for s in (f32(2 * rows, LANES), held(1, LANES), slab, held(sx, sy), slab, held(3, sx, sy), held(3, sx, sy))
        ],
        [held(rows, LANES), dma((2,))],
    )(vector, conductance)
    f = exchanged(f)
    (halo,) = call(halo_kernel, [IN_VMEM] * 5, [(held(3, sx, sy), IN_VMEM)])(r, c, u, keep, mid)
    halo = passed(halo, 1, count)
    (e,) = call(scan_kernel, [IN_VMEM] * 2, [(f32(2 * rows, LANES), IN_VMEM)])(f, d)
    e = exchanged(e)
    pe, we, q = call(
        early_kernel,
        [IN_HBM] + [IN_VMEM] * 4 + [IN_HBM],
        [(slab, IN_VMEM), (slab, IN_VMEM), (held(*krylov_basis.shape), IN_VMEM)],
        [slab, dma((2,))],
    )(vector, c, u, keep, halo, krylov_basis)
    p, w, dots = call(
        up_kernel,
        [IN_VMEM] * 5,
        [(slab, IN_VMEM), (slab, IN_VMEM), (f32(count, LANES), IN_VMEM)],
        [held(sx, sy), held(sx, sy)],
    )(e, c, pe, we, q)
    dots = exchanged(dots)
    p, following, coefficients = call(
        functools.partial(finish_kernel, cells),
        [IN_VMEM] * 4,
        [(out, IN_HBM), (out, IN_HBM), (pltpu.HBM((9,), jnp.float32), IN_HBM)],
        [slab, held(9), dma((6,))],
    )(dots, w, q, p)
    return (p, following, coefficients)


def solution(mesh):
    return jax.shard_map(
        on_device,
        mesh=mesh,
        in_specs=(P(None, TM, None, None), P(TM, None, None), P()),
        out_specs=(P(TM, None, None), P(TM, None, None), P()),
        check_vma=False,
    )
```
